256 devices in a mesh: dp: 64 (over x, z_lo, y, core), mp: 4 (over z_hi).
Axes of the slice: x: 4, y: 4, z: 8 (z_hi: 4, z_lo: 2; z = z_hi * 2 + z_lo), core: 2. Of those that a mesh axis runs over, the one named last changes fastest.
Arguments:
- pooled: bfloat16 [16384, 3584], P('dp', 'mp'), may hold values from -4 to 4
- w_out: bfloat16 [3584, 3584], P('mp'), may hold values from -0.028931878 to 0.028931878
- assignments: int32 [16384], P('dp'), may hold values from 0 to 4095
- ema_sums: float32 [4096, 3584], P('mp', 'dp'), may hold values from -0.40089186 to 0.40089186
- ema_counts: float32 [4096], P('mp'), may hold values from 1 to 8
Outputs:
- distances: float32 [16384, 4096], P('dp', 'mp')
- new_sums: float32 [4096, 3584], P('mp', 'dp')
- new_counts: float32 [4096], P('mp')
- new_centroids: bfloat16 [4096, 3584], P('mp', 'dp')
The draws below stay inside these ranges and needn't reach their ends.
All inputs are finite; a program needn't handle non-finite values.
Results may differ from the reference program's by a relative error of at most 0.0011.
Values may be sent and summed in bfloat16 or wider, within the bound.
No kernel may reach another device: no remote copies, remote signals or barrier semaphores. Data moves between devices by JAX's collectives and lax.ppermute only.
A program may use at most 64 MiB of HBM per device.

```python
import jax
import jax.numpy as jnp
from jax import lax

D = 3584
K = 4096
DOCS = 16384


def weight_matrix(key):
    bound_value = 0.99 * (3.0 / D) ** 0.5
    return jax.random.uniform(jax.random.fold_in(key, 101), (D, D), jnp.float32, -bound_value, bound_value)


def pooled_common(key):
    bound_value = 3.0 ** 0.5
    return jax.random.uniform(jax.random.fold_in(key, 102), (D,), jnp.float32, -bound_value, bound_value)


def embedded_common(key):
    projected = jnp.dot(pooled_common(key), weight_matrix(key), precision=lax.Precision.HIGHEST)
    return projected / jnp.sqrt(jnp.sum(projected * projected))


def count_values(key):
    return jnp.exp(jax.random.uniform(jax.random.fold_in(key, 103), (K,), jnp.float32, 0.0, jnp.log(8.0)))


def draw_w_out(key, part):
    return weight_matrix(key).astype(jnp.bfloat16)


def draw_pooled(key, part):
    noise_key = jax.random.fold_in(key, 104)
    loading_key = jax.random.fold_in(key, 105)
    noise_part = jax.random.normal(noise_key, (DOCS, D), jnp.float32)
    loadings = jax.random.uniform(loading_key, (DOCS, 1), jnp.float32, -1.5, 1.5)
    drawn_values = jnp.clip(noise_part + loadings * pooled_common(key)[None, :], -4.0, 4.0)
    return drawn_values.astype(jnp.bfloat16)


def draw_ema_counts(key, part):
    return count_values(key)


def draw_ema_sums(key, part):
    member_counts = count_values(key)
    shared_dir = embedded_common(key)
    random_part = jax.random.normal(jax.random.fold_in(key, 106), (K, D), jnp.float32)
    along_shared = jnp.sum(random_part * shared_dir[None, :], axis=1, keepdims=True)
    random_part = random_part - along_shared * shared_dir[None, :]
    random_part = random_part / jnp.sqrt(jnp.sum(random_part * random_part, axis=1, keepdims=True))
    alignment = jax.random.uniform(jax.random.fold_in(key, 107), (K, 1), jnp.float32, -0.9, 0.9)
    radius = jax.random.uniform(jax.random.fold_in(key, 108), (K, 1), jnp.float32, 0.3, 1.0)
    direction = radius * (alignment * shared_dir[None, :] + jnp.sqrt(1.0 - alignment * alignment) * random_part)
    bound_value = 24.0 * D ** (-0.5)
    return jnp.clip(member_counts[:, None] * direction, -bound_value, bound_value)


def place_ends(drawn, stream_key, least, largest):
    dims = drawn.shape
    index_at = [jax.random.randint(jax.random.fold_in(stream_key, axis), (), 0, dims[axis]) for axis in range(len(dims))]
    drawn = drawn.at[tuple(index_at)].set(least)
    longest = dims.index(max(dims))
    index_at[longest] = (index_at[longest] + 1) % dims[longest]
    return drawn.at[tuple(index_at)].set(largest)


def setup_inputs(seed: int = 0) -> dict:
    key_list = jax.random.split(jax.random.key(seed), 6)
    return {
        "pooled": draw_pooled(jax.random.fold_in(key_list[5], 71), 0),
        "w_out": draw_w_out(jax.random.fold_in(key_list[5], 71), 0),
        "assignments": place_ends(jax.random.randint(key_list[2], (DOCS,), 0, K), jax.random.fold_in(key_list[2], 1), 0, K - 1).astype(jnp.int32),
        "ema_sums": draw_ema_sums(jax.random.fold_in(key_list[5], 71), 0),
        "ema_counts": draw_ema_counts(jax.random.fold_in(key_list[5], 71), 0),
    }


def reference(pooled, w_out, assignments, ema_sums, ema_counts):
    proj = jnp.dot(pooled, w_out, preferred_element_type=jnp.float32)
    inverse_norm = 1.0 / jnp.sqrt(lax.optimization_barrier(jnp.sum(proj * proj, axis=1, keepdims=True)) + 1e-06)
    embedded = (proj * inverse_norm).astype(jnp.bfloat16)
    centers = (ema_sums / ema_counts[:, None]).astype(jnp.bfloat16)
    embed_wide = embedded.astype(jnp.float32)
    center_wide = centers.astype(jnp.float32)
    doc_norms = lax.optimization_barrier(jnp.sum(embed_wide * embed_wide, axis=1))
    center_norms = lax.optimization_barrier(jnp.sum(center_wide * center_wide, axis=1))
    products = jnp.dot(embedded, centers.T, preferred_element_type=jnp.float32)
    distances = doc_norms[:, None] + center_norms[None, :] - 2.0 * products
    batch_sums = jax.ops.segment_sum(embed_wide, assignments, num_segments=K)
    batch_counts = jax.ops.segment_sum(jnp.ones(assignments.shape, jnp.float32), assignments, num_segments=K)
    new_counts = 0.9 * ema_counts + 0.1 * batch_counts
    new_sums = 0.9 * ema_sums + 0.1 * batch_sums
    new_centroids = (new_sums / new_counts[:, None]).astype(jnp.bfloat16)
    return (distances, new_sums, new_counts, new_centroids)
```

```python
import functools

import jax
import jax.numpy as jnp
from jax import lax
from jax.experimental import pallas as pl
from jax.experimental.pallas import tpu as pltpu
from jax.sharding import PartitionSpec as P

EPSILON = 1e-06
EMA_DECAY = 0.9
CHUNKS = 2
SCALE = 64.0
MP = 4
GRID = (4, 2, 4, 2)


def mp_shift(value, step):
    return lax.ppermute(value, "mp", [(i, (i + step) % MP) for i in range(MP)])


def dp_index(place):
    index = 0
    for size, at in zip(GRID, place):
        index = index * size + at % size
    return index


def dp_shift(value, dim, step):
    pairs = []
    for index in range(64):
        rest, place = index, []
        for size in reversed(GRID):
            place.insert(0, rest % size)
            rest //= size
        moved = list(place)
        moved[dim] += step
        pairs.append((index, dp_index(moved)))
    return lax.ppermute(value, "dp", pairs)


def put(whole, piece, at):
    return lax.dynamic_update_slice_in_dim(whole, piece, at, 0)


def ring_of_four(piece, dim, at):
    size = GRID[dim]
    whole = jnp.zeros((size, *piece.shape), piece.dtype)
    whole = put(whole, piece[None], at)
    for step in (1, -1, 2):
        came = dp_shift(piece, dim, step)
        whole = put(whole, came[None], (at - step) % size)
    return whole


def gather_centers(piece):
    rows, wide = piece.shape
    index = lax.axis_index("dp")
    core, y, low, x = index % 2, index // 2 % 4, index // 8 % 2, index // 16
    with jax.named_scope("cz"):
        other = dp_shift(piece, 1, 1)
        pair = jnp.where(low == 0, jnp.stack([piece, other]), jnp.stack([other, piece]))
    with jax.named_scope("cy"):
        plane = ring_of_four(pair, 2, y)
    with jax.named_scope("cx"):
        block = ring_of_four(plane, 0, x)
    with jax.named_scope("cc"):
        other = dp_shift(block, 3, 1)
        first = jnp.where(core == 0, block, other)
        second = jnp.where(core == 0, other, block)
        both = jnp.stack([first, second])
    return jnp.transpose(both, (1, 3, 2, 0, 4, 5)).reshape(64 * rows, wide)


def sums_kernel(first_ref, assign_ref, cols_ref, out_ref):
    group, rows, docs = cols_ref.shape
    width = out_ref.shape[0]

    @pl.when(pl.program_id(0) == 0)
    def _():
        out_ref[...] = jnp.zeros_like(out_ref)

    ids = first_ref[0] + lax.broadcasted_iota(jnp.int32, (width, docs * group), 0)
    assign = jnp.concatenate([assign_ref[i] for i in range(group)], axis=1)
    hot = jnp.where(assign == ids, 1.0, 0.0).astype(jnp.bfloat16)
    cols = jnp.concatenate([cols_ref[i] for i in range(group)], axis=1)
    ones = jnp.ones((8, docs * group), jnp.bfloat16)
    cols = jnp.concatenate([cols, ones], axis=0)
    out_ref[...] += lax.dot_general(hot, cols, (((1,), (1,)), ((), ())), preferred_element_type=jnp.float32)


def batch_sums(first, assign, cols, width):
    shards, rows, docs = cols.shape
    group = max(1, 256 // docs)
    return pl.pallas_call(
        sums_kernel,
        grid_spec=pltpu.PrefetchScalarGridSpec(
            num_scalar_prefetch=1,
            grid=(shards // group,),
            in_specs=[
                pl.BlockSpec((group, 1, docs), lambda i, f: (i, 0, 0)),
                pl.BlockSpec((group, rows, docs), lambda i, f: (i, 0, 0)),
            ],
            out_specs=pl.BlockSpec((width, rows + 8), lambda i, f: (0, 0)),
        ),
        out_shape=jax.ShapeDtypeStruct((width, rows + 8), jnp.float32),
        cost_estimate=pl.CostEstimate(
            flops=2 * width * shards * docs * 256, bytes_accessed=2 * shards * rows * docs, transcendentals=0
        ),
        name="batch_sums",
    )(first, assign, cols)


def reduce_scatter(partial, me):
    docs, cols = partial.shape[0], partial.shape[1] // MP
    half = docs // 2

    def block(step):
        return lax.dynamic_slice_in_dim(partial, (me + step) % MP * cols, cols, 1)

    far = block(2).astype(jnp.float16)
    up = mp_shift(far[:half], 1).astype(jnp.float32)
    down = mp_shift(far[half:], -1).astype(jnp.float32)
    ahead, behind = block(1), block(-1)
    ahead = jnp.concatenate([ahead[:half] + up, ahead[half:]]).astype(jnp.float16)
    behind = jnp.concatenate([behind[:half], behind[half:] + down]).astype(jnp.float16)
    ahead = mp_shift(ahead, 1).astype(jnp.float32)
    behind = mp_shift(behind, -1).astype(jnp.float32)
    return block(0) + ahead + behind


def gather_pieces(piece):
    half = piece.shape[0] // 2
    behind = mp_shift(piece, 1)
    ahead = mp_shift(piece, -1)
    far_top = mp_shift(behind[:half], 1)
    far_low = mp_shift(ahead[half:], -1)
    return [(0, 0, piece), (-1, 0, behind), (1, 0, ahead), (2, 0, far_top), (2, half, far_low)]


def body(pooled, w_out, assignments, ema_sums, ema_counts):
    me = lax.axis_index("mp")
    docs = pooled.shape[0]
    width, feature_cols = ema_sums.shape
    shards = lax.axis_size("dp")

    sums_t = ema_sums.T
    with jax.named_scope("centers"):
        centers = (sums_t / ema_counts[None, :]).astype(jnp.bfloat16)
        centers = gather_centers(centers)
        wide = centers.astype(jnp.float32)
        center_norms = jnp.sum(wide * wide, axis=0)

    with jax.named_scope("assign"):
        copies = jnp.broadcast_to(assignments, (shards, 1, docs))
        every_assign = lax.all_to_all(copies, "dp", split_axis=0, concat_axis=0, tiled=True)

    chunk = docs // CHUNKS
    first = (me * width).reshape(1)
    embedded, received = [], []
    for i in range(CHUNKS):
        with jax.named_scope(f"proj{i}"):
            rows = pooled[i * chunk : (i + 1) * chunk]
            partial = jnp.dot(rows, w_out, preferred_element_type=jnp.float32) * SCALE
        with jax.named_scope(f"rs{i}"):
            share = reduce_scatter(partial, me)
        with jax.named_scope(f"ag{i}"):
            piece = share.T.astype(jnp.float16)
            pieces = gather_pieces(piece)
        with jax.named_scope(f"norm{i}"):
            pieces = [(s, o, p.astype(jnp.float32)) for s, o, p in pieces]
            squares = sum(jnp.sum(p * p, axis=0) for _, _, p in pieces)
            inverse = lax.rsqrt(squares + EPSILON * SCALE * SCALE)
            whole = jnp.zeros((MP * piece.shape[0], chunk), jnp.bfloat16)
            for s, o, p in pieces:
                at = (me + s) % MP * piece.shape[0] + o
                whole = put(whole, (p * inverse[None, :]).astype(jnp.bfloat16), at)
            embedded.append(whole)
        with jax.named_scope(f"out{i}"):
            cols = lax.all_to_all(
                whole.reshape(shards, feature_cols, chunk), "dp", split_axis=0, concat_axis=0, tiled=True
            )
            received.append(cols)
    with jax.named_scope("dist"):
        parts = []
        for whole in embedded:
            wide = whole.astype(jnp.float32)
            doc_norms = jnp.sum(wide * wide, axis=0)
            products = lax.dot_general(
                whole, centers, (((0,), (0,)), ((), ())), preferred_element_type=jnp.float32
            )
            parts.append(doc_norms[:, None] + center_norms[None, :] - 2.0 * products)
        distances = jnp.concatenate(parts)
    with jax.named_scope("sums"):
        total = 0.0
        for i, cols in enumerate(received):
            assign = every_assign[:, :, i * chunk : (i + 1) * chunk]
            total = total + batch_sums(first, assign, cols, width)
        total = total.T
        new_counts = EMA_DECAY * ema_counts + (1.0 - EMA_DECAY) * total[feature_cols]
        new_sums = EMA_DECAY * sums_t + (1.0 - EMA_DECAY) * total[:feature_cols]
        new_centroids = (new_sums / new_counts[None, :]).astype(jnp.bfloat16)
    return distances, new_sums.T, new_counts, new_centroids.T


def solution(mesh):
    return jax.shard_map(
        body,
        mesh=mesh,
        in_specs=(P("dp", "mp"), P("mp", None), P("dp"), P("mp", "dp"), P("mp")),
        out_specs=(P("dp", "mp"), P("mp", "dp"), P("mp"), P("mp", "dp")),
        check_vma=False,
    )
```

```python
import jax
import jax.numpy as jnp
from jax import lax
from jax.experimental import pallas as pl
from jax.experimental.pallas import tpu as pltpu
from jax.sharding import PartitionSpec as P

EPSILON = 1e-06
EMA_DECAY = 0.9
SCALE = 64.0
MP = 4
GRID = (4, 2, 4, 2)
LANES = 128


def mp_shift(value, step):
    return lax.ppermute(value, "mp", [(i, (i + step) % MP) for i in range(MP)])


def dp_index(place):
    index = 0
    for size, at in zip(GRID, place):
        index = index * size + at % size
    return index


def dp_shift(value, dim, step):
    pairs = []
    for index in range(64):
        rest, place = index, []
        for size in reversed(GRID):
            place.insert(0, rest % size)
            rest //= size
        moved = list(place)
        moved[dim] += step
        pairs.append((index, dp_index(moved)))
    return lax.ppermute(value, "dp", pairs)


def gather_table(piece):
    with jax.named_scope("cz"):
        pair = jnp.stack([piece, dp_shift(piece, 1, 1)])
    with jax.named_scope("cy"):
        line = jnp.stack([pair] + [dp_shift(pair, 2, -step) for step in (1, 2, 3)])
    with jax.named_scope("cx"):
        plane = jnp.stack([line] + [dp_shift(line, 0, -step) for step in (1, 2, 3)])
    with jax.named_scope("cc"):
        other = dp_shift(plane, 3, 1)
    return plane, other


def table_order(index):
    my = (index // 16, index // 8 % 2, index // 2 % 4, index % 2)
    i = jnp.arange(64, dtype=jnp.int32)
    x, low, y, core = (my[0] + i // 8) % 4, (my[1] + i) % 2, (my[2] + i // 2) % 4, (my[3] + i // 32) % 2
    blocks = ((x * 2 + low) * 4 + y) * 2 + core
    x, low, y, core = (i // 16 - my[0]) % 4, (i // 8 - my[1]) % 2, (i // 2 - my[2]) % 4, (i - my[3]) % 2
    entries = ((core * 4 + x) * 4 + y) * 2 + low
    return blocks.astype(jnp.int32), entries.astype(jnp.int32)


def place_kernel(at_ref, blocks_ref, *refs):
    pieces, (out_ref, order_ref, norms_ref) = refs[:-3], refs[-3:]
    rows, docs = pieces[0].shape
    step = 64
    norms = jnp.zeros((8, docs), jnp.float32)
    for i, piece in enumerate(pieces):
        for r in range(0, rows, step):
            e = piece[r : r + step, :]
            wide = e.astype(jnp.float32)
            norms += jnp.sum((wide * wide).reshape(step // 8, 8, docs), axis=0)
            out_ref[pl.ds(pl.multiple_of(at_ref[i] + r, 64), step), :] = e
    norms_ref[...] = jnp.sum(norms, axis=0, keepdims=True)
    cols, tall = out_ref.shape[0] // 64, order_ref.shape[0] // 64
    zeros = jnp.zeros((tall - cols, docs), jnp.bfloat16)
    for i in range(64):
        block = out_ref[pl.ds(pl.multiple_of(blocks_ref[i] * cols, 8), cols), :]
        order_ref[i * tall : i * tall + cols, :] = block
        order_ref[i * tall + cols : (i + 1) * tall, :] = zeros


def put_in_order(at, blocks, pieces):
    rows, docs = pieces[0].shape
    total = rows * len(pieces)
    whole = pl.BlockSpec(memory_space=pltpu.VMEM)
    return pl.pallas_call(
        place_kernel,
        grid_spec=pltpu.PrefetchScalarGridSpec(
            num_scalar_prefetch=2,
            grid=(),
            in_specs=[whole] * len(pieces),
            out_specs=[whole] * 3,
        ),
        out_shape=[
            jax.ShapeDtypeStruct((total, docs), jnp.bfloat16),
            jax.ShapeDtypeStruct((total + 64 * 8, docs), jnp.bfloat16),
            jax.ShapeDtypeStruct((1, docs), jnp.float32),
        ],
        cost_estimate=pl.CostEstimate(flops=3_000_000, bytes_accessed=6 * total * docs, transcendentals=0),
        name="put_in_order",
    )(at, blocks, *pieces)


def sums_kernel(first_ref, entries_ref, codes_ref, cols_ref, out_ref):
    group, rows, docs = cols_ref.shape
    tall = rows + 8
    blocks = out_ref.shape[1] // LANES

    @pl.when(pl.program_id(0) == 0)
    def _():
        out_ref[...] = jnp.zeros_like(out_ref)

    assign = []
    for i in range(group):
        codes = codes_ref[entries_ref[pl.program_id(0) * group + i]].astype(jnp.float32)
        assign.append(codes[0:1, :docs] * 64.0 + codes[0:1, docs:])
    assign = jnp.concatenate(assign, axis=1).astype(jnp.int32) - first_ref[0]
    high, low = assign >> 7, assign & (LANES - 1)
    ids = lax.broadcasted_iota(jnp.int32, (LANES, docs * group), 0)
    hot = jnp.where(low == ids, 1.0, 0.0).astype(jnp.bfloat16)
    cols = jnp.concatenate([cols_ref[i] for i in range(group)], axis=1)
    ones = jnp.ones((8, docs * group), jnp.bfloat16)
    cols = jnp.concatenate([cols, ones], axis=0)
    picked = []
    for b in range(blocks):
        mask = jnp.where(high == b, 1.0, 0.0).astype(jnp.bfloat16)
        picked.append(cols * mask)
    picked = jnp.concatenate(picked, axis=0)
    got = lax.dot_general(picked, hot, (((1,), (1,)), ((), ())), preferred_element_type=jnp.float32)
    for b in range(blocks):
        out_ref[:, b * LANES : (b + 1) * LANES] += got[b * tall : (b + 1) * tall]


def batch_sums(first, entries, codes, cols, width):
    shards, rows, docs = cols.shape
    group = 8
    return pl.pallas_call(
        sums_kernel,
        grid_spec=pltpu.PrefetchScalarGridSpec(
            num_scalar_prefetch=2,
            grid=(shards // group,),
            in_specs=[
                pl.BlockSpec(codes.shape, lambda i, f, e: (0, 0, 0)),
                pl.BlockSpec((group, rows, docs), lambda i, f, e: (i, 0, 0)),
            ],
            out_specs=pl.BlockSpec((rows + 8, width), lambda i, f, e: (0, 0)),
        ),
        out_shape=jax.ShapeDtypeStruct((rows + 8, width), jnp.float32),
        cost_estimate=pl.CostEstimate(
            flops=2 * width * shards * docs * rows, bytes_accessed=2 * shards * rows * docs, transcendentals=0
        ),
        name="batch_sums",
    )(first, entries, codes, cols)


def body(pooled, w_out, assignments, ema_sums, ema_counts):
    me = lax.axis_index("mp")
    index = lax.axis_index("dp")
    blocks, entries = table_order(index)
    docs, depth = pooled.shape
    half_docs, half = docs // 2, depth // 2
    width, feature_cols = ema_sums.shape
    shards = lax.axis_size("dp")
    f16 = jnp.float16

    def partial(step):
        w = lax.dynamic_slice_in_dim(w_out, (me + step) % MP * depth, depth, 1)
        return jnp.dot(pooled, w, preferred_element_type=jnp.float32) * SCALE

    with jax.named_scope("far"):
        far = partial(2).astype(f16)
    with jax.named_scope("rs1"):
        up = mp_shift(far[:half_docs], 1)
        down = mp_shift(far[half_docs:], -1)
    with jax.named_scope("near"):
        ahead, behind = partial(1), partial(-1)
    with jax.named_scope("rs2"):
        low_a = mp_shift(ahead[half_docs:].astype(f16), 1)
        top_b = mp_shift(behind[:half_docs].astype(f16), -1)
    with jax.named_scope("own"):
        mine = partial(0)
    with jax.named_scope("rs3"):
        top_a = mp_shift((ahead[:half_docs] + up.astype(jnp.float32)).astype(f16), 1)
        low_b = mp_shift((behind[half_docs:] + down.astype(jnp.float32)).astype(f16), -1)
    with jax.named_scope("share"):
        top = mine[:half_docs] + top_a.astype(jnp.float32) + top_b.astype(jnp.float32)
        low = mine[half_docs:] + low_a.astype(jnp.float32) + low_b.astype(jnp.float32)
        share = jnp.concatenate([top, low]).T.astype(f16)
        first_half, second_half = share[:half], share[half:]
    with jax.named_scope("ag1"):
        a_first = mp_shift(first_half, 1)
        b_second = mp_shift(second_half, -1)
    with jax.named_scope("ag2"):
        a_second = mp_shift(second_half, 1)
        b_first = mp_shift(first_half, -1)
    with jax.named_scope("ag3"):
        c_first = mp_shift(a_first, 1)
        c_second = mp_shift(b_second, -1)

    sums_t = ema_sums.T
    with jax.named_scope("centers"):
        centers = (sums_t / ema_counts[None, :]).astype(jnp.bfloat16)
        pair = jnp.stack([assignments // 64, assignments % 64]).astype(jnp.bfloat16).reshape(1, 2 * docs)
        extra = jnp.pad(pair, ((0, 7), (0, width - 2 * docs)))
        tables = gather_table(jnp.concatenate([centers, extra]))
        tables = [t.reshape(shards // 2, feature_cols + 8, width) for t in tables]
        real = lax.broadcasted_iota(jnp.int32, tables[0].shape, 1) < feature_cols
        center_norms = 0.0
        for table in tables:
            wide = jnp.where(real, table.astype(jnp.float32), 0.0)
            center_norms = center_norms + jnp.sum(wide * wide, axis=(0, 1))
    with jax.named_scope("codes"):
        codes = jnp.concatenate([t[:, feature_cols:, : 2 * docs] for t in tables])

    with jax.named_scope("norm"):
        parts = [
            first_half, second_half, b_first, b_second, c_first, c_second, a_first, a_second
        ]
        i = jnp.arange(len(parts), dtype=jnp.int32)
        at = ((me + i // 2) % MP * depth + i % 2 * half).astype(jnp.int32)
        wide = [p.astype(jnp.float32) for p in parts]
        squares = sum(jnp.sum(p * p, axis=0) for p in wide)
        inverse = lax.rsqrt(squares + EPSILON * SCALE * SCALE)
        pieces = [(p * inverse[None, :]).astype(jnp.bfloat16) for p in wide]
        embedded, ordered, doc_norms = put_in_order(at, blocks, pieces)
    with jax.named_scope("out"):
        received = lax.all_to_all(
            embedded.reshape(shards, feature_cols, docs), "dp", split_axis=0, concat_axis=0, tiled=True
        )
    with jax.named_scope("dist"):
        products = 0.0
        for i, table in enumerate(tables):
            rows = table.reshape(-1, width)
            part = ordered[i * rows.shape[0] : (i + 1) * rows.shape[0]]
            products = products + lax.dot_general(
                part, rows, (((0,), (0,)), ((), ())), preferred_element_type=jnp.float32
            )
        distances = doc_norms[0][:, None] + center_norms[None, :] - 2.0 * products
    received, distances = lax.optimization_barrier((received, distances))
    with jax.named_scope("sums"):
        total = batch_sums((me * width).reshape(1), entries, codes, received, width)
        new_counts = EMA_DECAY * ema_counts + (1.0 - EMA_DECAY) * total[feature_cols]
        new_sums = EMA_DECAY * sums_t + (1.0 - EMA_DECAY) * total[:feature_cols]
        new_centroids = (new_sums / new_counts[None, :]).astype(jnp.bfloat16)
    return distances, new_sums.T, new_counts, new_centroids.T


def solution(mesh):
    return jax.shard_map(
        body,
        mesh=mesh,
        in_specs=(P("dp", "mp"), P("mp", None), P("dp"), P("mp", "dp"), P("mp")),
        out_specs=(P("dp", "mp"), P("mp", "dp"), P("mp"), P("mp", "dp")),
        check_vma=False,
    )
```

```python
import jax
import jax.numpy as jnp
from jax import lax
from jax.experimental import pallas as pl
from jax.experimental.pallas import tpu as pltpu
from jax.sharding import PartitionSpec as P


EPSILON = 1e-06
EMA_DECAY = 0.9
SCALE = 64.0
MP = 4
GRID = (4, 2, 4, 2)
LANES = 256


def mp_shift(value, step):
    return lax.ppermute(value, "mp", [(i, (i + step) % MP) for i in range(MP)])


def after(values, *others):
    return lax.optimization_barrier((values, others))[0]


def dp_index(place):
    index = 0
    for size, at in zip(GRID, place):
        index = index * size + at % size
    return index


def dp_shift(value, dim, step):
    pairs = []
    for index in range(64):
        rest, place = index, []
        for size in reversed(GRID):
            place.insert(0, rest % size)
            rest //= size
        moved = list(place)
        moved[dim] += step
        pairs.append((index, dp_index(moved)))
    return lax.ppermute(value, "dp", pairs)


def gather_line(piece, hold):
    pair = jnp.stack([piece, after(dp_shift(piece, 1, 1), hold)])
    return [pair] + [dp_shift(pair, 2, -step) for step in (1, 2, 3)]


def gather_plane(line, hold):
    line = jnp.stack(after(line, hold))
    return [line] + [dp_shift(line, 0, -step) for step in (1, 2, 3)]


def gather_table(plane, hold):
    plane = jnp.stack(after(plane, hold))
    return plane, dp_shift(plane, 3, 1)


def table_order(index):
    my = (index // 16, index // 8 % 2, index // 2 % 4, index % 2)
    i = jnp.arange(64, dtype=jnp.int32)
    x, low, y, core = (my[0] + i // 8) % 4, (my[1] + i) % 2, (my[2] + i // 2) % 4, (my[3] + i // 32) % 2
    blocks = ((x * 2 + low) * 4 + y) * 2 + core
    x, low, y, core = (i // 16 - my[0]) % 4, (i // 8 - my[1]) % 2, (i // 2 - my[2]) % 4, (i - my[3]) % 2
    entries = ((core * 4 + x) * 4 + y) * 2 + low
    return blocks.astype(jnp.int32), entries.astype(jnp.int32)


def place_kernel(at_ref, *refs):
    pieces, out_ref = refs[:-1], refs[-1]
    rows = pieces[0].shape[0]
    for i, piece in enumerate(pieces):
        out_ref[pl.ds(pl.multiple_of(at_ref[i], 64), rows), :] = piece[...]


def put_in_place(at, pieces):
    rows, docs = pieces[0].shape
    total = rows * len(pieces)
    whole = pl.BlockSpec(memory_space=pltpu.VMEM)
    return pl.pallas_call(
        place_kernel,
        grid_spec=pltpu.PrefetchScalarGridSpec(
            num_scalar_prefetch=1, grid=(), in_specs=[whole] * len(pieces), out_specs=whole
        ),
        out_shape=jax.ShapeDtypeStruct((total, docs), jnp.bfloat16),
        cost_estimate=pl.CostEstimate(flops=1_000_000, bytes_accessed=4 * total * docs, transcendentals=0),
        name="put_in_place",
    )(at, *pieces)


def order_kernel(blocks_ref, whole_ref, order_ref, norms_ref):
    docs = whole_ref.shape[1]
    cols, tall = whole_ref.shape[0] // 64, order_ref.shape[0] // 64
    zeros = jnp.zeros((tall - cols, docs), jnp.bfloat16)
    norms = jnp.zeros((8, docs), jnp.float32)
    for i in range(64):
        block = whole_ref[pl.ds(pl.multiple_of(blocks_ref[i] * cols, 8), cols), :]
        wide = block.astype(jnp.float32)
        norms += jnp.sum((wide * wide).reshape(cols // 8, 8, docs), axis=0)
        order_ref[i * tall : i * tall + cols, :] = block
        order_ref[i * tall + cols : (i + 1) * tall, :] = zeros
    norms_ref[...] = jnp.sum(norms, axis=0, keepdims=True)


def put_in_order(blocks, whole):
    rows, docs = whole.shape
    vmem = pl.BlockSpec(memory_space=pltpu.VMEM)
    return pl.pallas_call(
        order_kernel,
        grid_spec=pltpu.PrefetchScalarGridSpec(num_scalar_prefetch=1, grid=(), in_specs=[vmem], out_specs=[vmem] * 2),
        out_shape=[
            jax.ShapeDtypeStruct((rows + 64 * 8, docs), jnp.bfloat16),
            jax.ShapeDtypeStruct((1, docs), jnp.float32),
        ],
        cost_estimate=pl.CostEstimate(flops=3_000_000, bytes_accessed=4 * rows * docs, transcendentals=0),
        name="put_in_order",
    )(blocks, whole)


def sums_kernel(first_ref, entries_ref, codes_ref, cols_ref, ema_ref, counts_ref, sums_out, counts_out, means_out, total):
    group, rows, docs = cols_ref.shape
    tall = rows + 8
    blocks = total.shape[1] // LANES

    @pl.when(pl.program_id(0) == 0)
    def _():
        total[...] = jnp.zeros_like(total)

    assign = []
    for i in range(group):
        codes = codes_ref[entries_ref[pl.program_id(0) * group + i]].astype(jnp.float32)
        assign.append(codes[0:1, :docs] * 64.0 + codes[0:1, docs:])
    assign = jnp.concatenate(assign, axis=1).astype(jnp.int32) - first_ref[0]
    low = assign & (LANES - 1)
    high = assign - low
    ids = lax.broadcasted_iota(jnp.int32, (LANES, docs * group), 0)
    hot = jnp.where(low == ids, 1.0, 0.0).astype(jnp.bfloat16)
    cols = jnp.concatenate([cols_ref[i] for i in range(group)], axis=1)
    ones = jnp.ones((8, docs * group), jnp.bfloat16)
    cols = jnp.concatenate([cols, ones], axis=0)
    picked = []
    for b in range(blocks):
        mask = jnp.where(high == b * LANES, 1.0, 0.0).astype(jnp.bfloat16)
        picked.append(cols * mask)
    picked = jnp.concatenate(picked, axis=0)
    got = lax.dot_general(picked, hot, (((1,), (1,)), ((), ())), preferred_element_type=jnp.float32)
    for b in range(blocks):
        total[:, b * LANES : (b + 1) * LANES] += got[b * tall : (b + 1) * tall]

    @pl.when(pl.program_id(0) == pl.num_programs(0) - 1)
    def _():
        counts = EMA_DECAY * counts_ref[...] + (1.0 - EMA_DECAY) * total[rows : rows + 1]
        sums = EMA_DECAY * ema_ref[...] + (1.0 - EMA_DECAY) * total[:rows]
        counts_out[...] = counts
        sums_out[...] = sums
        means_out[...] = (sums / counts).astype(jnp.bfloat16)


def new_state(first, entries, codes, cols, ema_sums, ema_counts):
    shards, rows, docs = cols.shape
    width = ema_counts.shape[1]
    group = 8

    def all_of(shape):
        return pl.BlockSpec(shape, lambda i, f, e: (0,) * len(shape))

    return pl.pallas_call(
        sums_kernel,
        grid_spec=pltpu.PrefetchScalarGridSpec(
            num_scalar_prefetch=2,
            grid=(shards // group,),
            in_specs=[
                all_of(codes.shape),
                pl.BlockSpec((group, rows, docs), lambda i, f, e: (i, 0, 0)),
                all_of((rows, width)),
                all_of((1, width)),
            ],
            out_specs=[all_of((rows, width)), all_of((1, width)), all_of((rows, width))],
            scratch_shapes=[pltpu.VMEM((rows + 8, width), jnp.float32)],
        ),
        out_shape=[
            jax.ShapeDtypeStruct((rows, width), jnp.float32),
            jax.ShapeDtypeStruct((1, width), jnp.float32),
            jax.ShapeDtypeStruct((rows, width), jnp.bfloat16),
        ],
        cost_estimate=pl.CostEstimate(
            flops=2 * width * shards * docs * rows, bytes_accessed=2 * shards * rows * docs, transcendentals=0
        ),
        name="new_state",
    )(first, entries, codes, cols, ema_sums, ema_counts)


def step(pooled, w_out, assignments, ema_sums, ema_counts):
    me = lax.axis_index("mp")
    index = lax.axis_index("dp")
    blocks, entries = table_order(index)
    docs, depth = pooled.shape
    half_docs, half = docs // 2, depth // 2
    width, feature_cols = ema_sums.shape
    shards = lax.axis_size("dp")
    f16 = jnp.float16

    def partial(step):
        w = lax.dynamic_slice_in_dim(w_out, (me + step) % MP * depth, depth, 1)
        return jnp.dot(pooled, w, preferred_element_type=jnp.float32) * SCALE

    far = partial(2).astype(f16)
    up = mp_shift(far[:half_docs], 1)
    down = mp_shift(far[half_docs:], -1)
    sums_t = ema_sums.T
    centers = (sums_t / ema_counts[None, :]).astype(jnp.bfloat16)
    pair = jnp.stack([assignments // 64, assignments % 64]).astype(jnp.bfloat16).reshape(1, 2 * docs)
    extra = jnp.pad(pair, ((0, 7), (0, width - 2 * docs)))
    centers = after(jnp.concatenate([centers, extra]), far)
    ahead, behind = partial(1), partial(-1)
    low_a, top_b = ahead[half_docs:].astype(f16), behind[:half_docs].astype(f16)
    line = gather_line(centers, (low_a, top_b))
    near = (low_a, top_b)
    low_a, top_b = mp_shift(low_a, 1), mp_shift(top_b, -1)
    mine = partial(0)
    up, down = after((up, down), near, mine)
    top_a = (ahead[:half_docs] + up.astype(jnp.float32)).astype(f16)
    low_b = (behind[half_docs:] + down.astype(jnp.float32)).astype(f16)
    plane = gather_plane(line, (top_a, low_b))
    top_a, low_b = mp_shift(top_a, 1), mp_shift(low_b, -1)
    top = mine[:half_docs] + top_a.astype(jnp.float32) + top_b.astype(jnp.float32)
    low = mine[half_docs:] + low_a.astype(jnp.float32) + low_b.astype(jnp.float32)
    share = jnp.concatenate([top, low]).T.astype(f16)
    first_half, second_half = share[:half], share[half:]
    a_first = mp_shift(first_half, 1)
    b_second = mp_shift(second_half, -1)
    a_second = mp_shift(second_half, 1)
    b_first = mp_shift(first_half, -1)
    c_first = mp_shift(a_first, 1)
    c_second = mp_shift(b_second, -1)

    tables = gather_table(plane, (a_first, b_second, a_second, b_first))
    blocks, entries = table_order(index)
    parts = [first_half, second_half, b_first, b_second, c_first, c_second, a_first, a_second]
    i = jnp.arange(len(parts), dtype=jnp.int32)
    at = ((me + i // 2) % MP * depth + i % 2 * half).astype(jnp.int32)
    wide = [p.astype(jnp.float32) for p in parts]
    squares = sum(jnp.sum(p * p, axis=0) for p in wide)
    inverse = lax.rsqrt(squares + EPSILON * SCALE * SCALE)
    pieces = [(p * inverse[None, :]).astype(jnp.bfloat16) for p in wide]
    embedded = put_in_place(at, pieces)
    received = lax.all_to_all(
        embedded.reshape(shards, feature_cols, docs), "dp", split_axis=0, concat_axis=0, tiled=True
    )
    ordered, doc_norms = put_in_order(blocks, embedded)
    tables = [t.reshape(shards // 2, feature_cols + 8, width) for t in tables]
    codes = jnp.concatenate([t[:, feature_cols:, : 2 * docs] for t in tables])
    real = lax.broadcasted_iota(jnp.int32, tables[0].shape, 1) < feature_cols
    center_norms, products = 0.0, 0.0
    for i, table in enumerate(tables):
        wide = jnp.where(real, table.astype(jnp.float32), 0.0)
        center_norms = center_norms + jnp.sum(wide * wide, axis=(0, 1))
        rows = table.reshape(-1, width)
        part = ordered[i * rows.shape[0] : (i + 1) * rows.shape[0]]
        products = products + lax.dot_general(part, rows, (((0,), (0,)), ((), ())), preferred_element_type=jnp.float32)
    distances = doc_norms[0][:, None] + center_norms[None, :] - 2.0 * products
    received, distances, codes = lax.optimization_barrier((received, distances, codes))
    new_sums, new_counts, new_centroids = new_state(
        (me * width).reshape(1), entries, codes, received, sums_t, ema_counts[None, :]
    )
    return distances, new_sums.T, new_counts[0], new_centroids.T


def solution(mesh):
    return jax.shard_map(
        step,
        mesh=mesh,
        in_specs=(P("dp", "mp"), P("mp", None), P("dp"), P("mp", "dp"), P("mp")),
        out_specs=(P("dp", "mp"), P("mp", "dp"), P("mp"), P("mp", "dp")),
        check_vma=False,
    )
```

```python
import jax
import jax.numpy as jnp
from jax import lax
from jax.experimental import pallas as pl
from jax.experimental.pallas import tpu as pltpu
from jax.sharding import PartitionSpec as P


EPSILON = 1e-06
EMA_DECAY = 0.9
SCALE = 64.0
MP = 4
GRID = (4, 2, 4, 2)
LANES = 256


def mp_shift(value, step):
    return lax.ppermute(value, "mp", [(i, (i + step) % MP) for i in range(MP)])


def after(values, *others):
    return lax.optimization_barrier((values, others))[0]


def dp_index(place):
    index = 0
    for size, at in zip(GRID, place):
        index = index * size + at % size
    return index


def dp_shift(value, dim, step):
    pairs = []
    for index in range(64):
        rest, place = index, []
        for size in reversed(GRID):
            place.insert(0, rest % size)
            rest //= size
        moved = list(place)
        moved[dim] += step
        pairs.append((index, dp_index(moved)))
    return lax.ppermute(value, "dp", pairs)


def shifts(value, dim):
    return [value] + [dp_shift(value, dim, -step) for step in (1, 2, 3)]


def first_lines(piece, hold):
    half = piece.shape[0] // 2
    pair = jnp.stack([piece, after(dp_shift(piece, 1, 1), hold)])
    return shifts(pair[:, :half], 2), shifts(pair[:, half:], 0)


def second_lines(upper, lower, hold):
    upper, lower = after((upper, lower), hold)
    return shifts(jnp.stack(upper), 0), shifts(jnp.stack(lower), 2)


def gather_tables(upper, lower, hold):
    upper, lower = after((upper, lower), hold)
    tables = [jnp.stack(upper), jnp.stack(lower)]
    return tables + [dp_shift(t, 3, 1) for t in tables]


def table_order(index):
    my = (index // 16, index // 8 % 2, index // 2 % 4, index % 2)
    i = jnp.arange(64, dtype=jnp.int32)

    def block(x, y):
        low, core = (my[1] + i) % 2, (my[3] + i // 32) % 2
        return (((my[0] + x) % 4 * 2 + low) * 4 + (my[2] + y) % 4) * 2 + core

    upper, lower = block(i // 8, i // 2), block(i // 2, i // 8)
    x, low, y, core = (i // 16 - my[0]) % 4, (i // 8 - my[1]) % 2, (i // 2 - my[2]) % 4, (i - my[3]) % 2
    entries = ((core * 4 + y) * 4 + x) * 2 + low
    return jnp.concatenate([upper, lower]).astype(jnp.int32), entries.astype(jnp.int32)


def place_kernel(at_ref, *refs):
    pieces, out_ref, sems = refs[:-2], refs[-2], refs[-1]
    rows = pieces[0].shape[0]
    copies = [
        pltpu.make_async_copy(piece, out_ref.at[pl.ds(pl.multiple_of(at_ref[i], 64), rows)], sems.at[i])
        for i, piece in enumerate(pieces)
    ]
    for copy in copies:
        copy.start()
    for copy in copies:
        copy.wait()


def put_in_place(at, pieces):
    rows, docs = pieces[0].shape
    total = rows * len(pieces)
    return pl.pallas_call(
        place_kernel,
        grid_spec=pltpu.PrefetchScalarGridSpec(
            num_scalar_prefetch=1,
            grid=(),
            in_specs=[pl.BlockSpec(memory_space=pltpu.VMEM)] * len(pieces),
            out_specs=pl.BlockSpec(memory_space=pl.ANY),
            scratch_shapes=[pltpu.SemaphoreType.DMA((len(pieces),))],
        ),
        out_shape=jax.ShapeDtypeStruct((total, docs), jnp.bfloat16),
        cost_estimate=pl.CostEstimate(flops=1_000_000, bytes_accessed=4 * total * docs, transcendentals=0),
        compiler_params=pltpu.CompilerParams(vmem_limit_bytes=4 * 1024 * 1024),
        name="put_in_place",
    )(at, *pieces)


def order_kernel(blocks_ref, whole_ref, order_ref, norms_ref):
    docs = whole_ref.shape[1]
    cols = whole_ref.shape[0] // 64
    upper = order_ref.shape[0] // 128
    zeros = jnp.zeros((2 * upper - cols, docs), jnp.bfloat16)
    norms = jnp.zeros((8, docs), jnp.float32)
    for part in range(4):
        rows, first = (upper, 0) if part % 2 == 0 else (cols - upper, upper)
        for i in range(32):
            block = blocks_ref[part % 2 * 64 + part // 2 * 32 + i]
            block = whole_ref[pl.ds(pl.multiple_of(block * cols + first, 8), rows), :]
            wide = block.astype(jnp.float32)
            norms += jnp.sum((wide * wide).reshape(rows // 8, 8, docs), axis=0)
            to = (part * 32 + i) * upper
            order_ref[to : to + rows, :] = block
            if rows < upper:
                order_ref[to + rows : to + upper, :] = zeros
    norms_ref[...] = jnp.sum(norms, axis=0, keepdims=True)


def put_in_order(blocks, whole):
    rows, docs = whole.shape
    vmem = pl.BlockSpec(memory_space=pltpu.VMEM)
    return pl.pallas_call(
        order_kernel,
        grid_spec=pltpu.PrefetchScalarGridSpec(num_scalar_prefetch=1, grid=(), in_specs=[vmem], out_specs=[vmem] * 2),
        out_shape=[
            jax.ShapeDtypeStruct((rows + 64 * 8, docs), jnp.bfloat16),
            jax.ShapeDtypeStruct((1, docs), jnp.float32),
        ],
        cost_estimate=pl.CostEstimate(flops=3_000_000, bytes_accessed=4 * rows * docs, transcendentals=0),
        name="put_in_order",
    )(blocks, whole)


def sums_kernel(first_ref, entries_ref, codes_ref, cols_ref, ema_ref, counts_ref, sums_out, counts_out, means_out, total):
    group, rows, docs = cols_ref.shape
    tall = rows + 8
    blocks = total.shape[1] // LANES

    @pl.when(pl.program_id(0) == 0)
    def _():
        total[...] = jnp.zeros_like(total)

    assign = []
    for i in range(group):
        codes = codes_ref[entries_ref[pl.program_id(0) * group + i]].astype(jnp.float32)
        assign.append(codes[0:1, :docs] * 64.0 + codes[0:1, docs:])
    assign = jnp.concatenate(assign, axis=1).astype(jnp.int32) - first_ref[0]
    low = assign & (LANES - 1)
    high = assign - low
    ids = lax.broadcasted_iota(jnp.int32, (LANES, docs * group), 0)
    hot = jnp.where(low == ids, 1.0, 0.0).astype(jnp.bfloat16)
    cols = jnp.concatenate([cols_ref[i] for i in range(group)], axis=1)
    ones = jnp.ones((8, docs * group), jnp.bfloat16)
    cols = jnp.concatenate([cols, ones], axis=0)
    picked = []
    for b in range(blocks):
        mask = jnp.where(high == b * LANES, 1.0, 0.0).astype(jnp.bfloat16)
        picked.append(cols * mask)
    picked = jnp.concatenate(picked, axis=0)
    got = lax.dot_general(picked, hot, (((1,), (1,)), ((), ())), preferred_element_type=jnp.float32)
    for b in range(blocks):
        total[:, b * LANES : (b + 1) * LANES] += got[b * tall : (b + 1) * tall]

    @pl.when(pl.program_id(0) == pl.num_programs(0) - 1)
    def _():
        counts = EMA_DECAY * counts_ref[...] + (1.0 - EMA_DECAY) * total[rows : rows + 1]
        sums = EMA_DECAY * ema_ref[...] + (1.0 - EMA_DECAY) * total[:rows]
        counts_out[...] = counts
        sums_out[...] = sums
        means_out[...] = (sums / counts).astype(jnp.bfloat16)


def new_state(first, entries, codes, cols, ema_sums, ema_counts):
    shards, rows, docs = cols.shape
    width = ema_counts.shape[1]
    group = 8

    def all_of(shape):
        return pl.BlockSpec(shape, lambda i, f, e: (0,) * len(shape))

    return pl.pallas_call(
        sums_kernel,
        grid_spec=pltpu.PrefetchScalarGridSpec(
            num_scalar_prefetch=2,
            grid=(shards // group,),
            in_specs=[
                all_of(codes.shape),
                pl.BlockSpec((group, rows, docs), lambda i, f, e: (i, 0, 0)),
                all_of((rows, width)),
                all_of((1, width)),
            ],
            out_specs=[all_of((rows, width)), all_of((1, width)), all_of((rows, width))],
            scratch_shapes=[pltpu.VMEM((rows + 8, width), jnp.float32)],
        ),
        out_shape=[
            jax.ShapeDtypeStruct((rows, width), jnp.float32),
            jax.ShapeDtypeStruct((1, width), jnp.float32),
            jax.ShapeDtypeStruct((rows, width), jnp.bfloat16),
        ],
        cost_estimate=pl.CostEstimate(
            flops=2 * width * shards * docs * rows, bytes_accessed=2 * shards * rows * docs, transcendentals=0
        ),
        name="new_state",
    )(first, entries, codes, cols, ema_sums, ema_counts)


def step(pooled, w_out, assignments, ema_sums, ema_counts):
    me = lax.axis_index("mp")
    index = lax.axis_index("dp")
    blocks, entries = table_order(index)
    docs, depth = pooled.shape
    half_docs, half = docs // 2, depth // 2
    width, feature_cols = ema_sums.shape
    shards = lax.axis_size("dp")
    f16 = jnp.float16

    def partial(step):
        w = lax.dynamic_slice_in_dim(w_out, (me + step) % MP * depth, depth, 1)
        return jnp.dot(pooled, w, preferred_element_type=jnp.float32) * SCALE

    far = partial(2).astype(f16)
    up = mp_shift(far[:half_docs], 1)
    down = mp_shift(far[half_docs:], -1)
    sums_t = ema_sums.T
    centers = (sums_t / ema_counts[None, :]).astype(jnp.bfloat16)
    pair = jnp.stack([assignments // 64, assignments % 64]).astype(jnp.bfloat16).reshape(1, 2 * docs)
    extra = jnp.pad(pair, ((0, 7), (0, width - 2 * docs)))
    centers = jnp.concatenate([centers, extra])
    ahead, behind = partial(1), partial(-1)
    low_a, top_b = ahead[half_docs:].astype(f16), behind[:half_docs].astype(f16)
    lines = first_lines(centers, (low_a, top_b))
    near = (low_a, top_b)
    low_a, top_b = mp_shift(low_a, 1), mp_shift(top_b, -1)
    mine = partial(0)
    up, down = after((up, down), near, mine)
    top_a = (ahead[:half_docs] + up.astype(jnp.float32)).astype(f16)
    low_b = (behind[half_docs:] + down.astype(jnp.float32)).astype(f16)
    lines = second_lines(*lines, (top_a, low_b))
    top_a, low_b = mp_shift(top_a, 1), mp_shift(low_b, -1)
    top = mine[:half_docs] + top_a.astype(jnp.float32) + top_b.astype(jnp.float32)
    low = mine[half_docs:] + low_a.astype(jnp.float32) + low_b.astype(jnp.float32)
    share = jnp.concatenate([top, low]).T.astype(f16)
    first_half, second_half = share[:half], share[half:]
    a_first = mp_shift(first_half, 1)
    b_second = mp_shift(second_half, -1)
    a_second = mp_shift(second_half, 1)
    b_first = mp_shift(first_half, -1)
    c_first = mp_shift(a_first, 1)
    c_second = mp_shift(b_second, -1)

    tables = gather_tables(*lines, (a_first, b_second, a_second, b_first))
    blocks, entries = table_order(index)
    parts = [first_half, second_half, b_first, b_second, c_first, c_second, a_first, a_second]
    i = jnp.arange(len(parts), dtype=jnp.int32)
    at = ((me + i // 2) % MP * depth + i % 2 * half).astype(jnp.int32)
    wide = [p.astype(jnp.float32) for p in parts]
    squares = sum(jnp.sum(p * p, axis=0) for p in wide)
    inverse = lax.rsqrt(squares + EPSILON * SCALE * SCALE)
    pieces = [(p * inverse[None, :]).astype(jnp.bfloat16) for p in wide]
    embedded = put_in_place(at, pieces)
    received = lax.all_to_all(
        embedded.reshape(shards, feature_cols, docs), "dp", split_axis=0, concat_axis=0, tiled=True
    )
    ordered, doc_norms = put_in_order(blocks, embedded)
    upper = (feature_cols + 8) // 2
    tables = [t.reshape(shards // 2, upper, width) for t in tables]
    real = feature_cols - upper
    codes = jnp.concatenate([t[:, real:, : 2 * docs] for t in tables[1::2]])
    center_norms, products = 0.0, 0.0
    for i, table in enumerate(tables):
        wide = table.astype(jnp.float32)
        if i % 2:
            wide = jnp.where(lax.broadcasted_iota(jnp.int32, table.shape, 1) < real, wide, 0.0)
        center_norms = center_norms + jnp.sum(wide * wide, axis=(0, 1))
        rows = table.reshape(-1, width)
        part = ordered[i * rows.shape[0] : (i + 1) * rows.shape[0]]
        products = products + lax.dot_general(part, rows, (((0,), (0,)), ((), ())), preferred_element_type=jnp.float32)
    distances = doc_norms[0][:, None] + center_norms[None, :] - 2.0 * products
    received, distances, codes = lax.optimization_barrier((received, distances, codes))
    new_sums, new_counts, new_centroids = new_state(
        (me * width).reshape(1), entries, codes, received, sums_t, ema_counts[None, :]
    )
    return distances, new_sums.T, new_counts[0], new_centroids.T


def solution(mesh):
    return jax.shard_map(
        step,
        mesh=mesh,
        in_specs=(P("dp", "mp"), P("mp", None), P("dp"), P("mp", "dp"), P("mp")),
        out_specs=(P("dp", "mp"), P("mp", "dp"), P("mp"), P("mp", "dp")),
        check_vma=False,
    )
```

```python
import jax
import jax.numpy as jnp
from jax import lax
from jax.experimental import pallas as pl
from jax.experimental.pallas import tpu as pltpu
from jax.sharding import PartitionSpec as P


EPSILON = 1e-06
EMA_DECAY = 0.9
SCALE = 64.0
MP = 4
GRID = (4, 2, 4, 2)
LANES = 256


def mp_shift(value, step):
    return lax.ppermute(value, "mp", [(i, (i + step) % MP) for i in range(MP)])


def after(values, *others):
    return lax.optimization_barrier((values, others))[0]


def dp_index(place):
    index = 0
    for size, at in zip(GRID, place):
        index = index * size + at % size
    return index


def dp_shift(value, dim, step):
    pairs = []
    for index in range(64):
        rest, place = index, []
        for size in reversed(GRID):
            place.insert(0, rest % size)
            rest //= size
        moved = list(place)
        moved[dim] += step
        pairs.append((index, dp_index(moved)))
    return lax.ppermute(value, "dp", pairs)


def shifts(value, dim):
    return [value] + [dp_shift(value, dim, -step) for step in (1, 2, 3)]


def first_lines(piece, hold):
    half = piece.shape[0] // 2
    pair = jnp.stack([piece, after(dp_shift(piece, 1, 1), hold)])
    return shifts(pair[:, :half], 2), shifts(pair[:, half:], 0)


def second_lines(upper, lower, hold):
    upper, lower = after((upper, lower), hold)
    return shifts(jnp.stack(upper), 0), shifts(jnp.stack(lower), 2)


def gather_tables(upper, lower, hold):
    upper, lower = after((upper, lower), hold)
    tables = [jnp.stack(upper), jnp.stack(lower)]
    return tables + [dp_shift(t, 3, 1) for t in tables]


def table_order(index):
    my = (index // 16, index // 8 % 2, index // 2 % 4, index % 2)
    i = jnp.arange(64, dtype=jnp.int32)

    def block(x, y):
        low, core = (my[1] + i) % 2, (my[3] + i // 32) % 2
        return (((my[0] + x) % 4 * 2 + low) * 4 + (my[2] + y) % 4) * 2 + core

    upper, lower = block(i // 8, i // 2), block(i // 2, i // 8)
    x, low, y, core = (i // 16 - my[0]) % 4, (i // 8 - my[1]) % 2, (i // 2 - my[2]) % 4, (i - my[3]) % 2
    entries = ((core * 4 + y) * 4 + x) * 2 + low
    return jnp.concatenate([upper, lower]).astype(jnp.int32), entries.astype(jnp.int32)


def place_kernel(at_ref, *refs):
    pieces, out_ref, sems = refs[:-2], refs[-2], refs[-1]
    rows = pieces[0].shape[0]
    copies = [
        pltpu.make_async_copy(piece, out_ref.at[pl.ds(pl.multiple_of(at_ref[i], 64), rows)], sems.at[i])
        for i, piece in enumerate(pieces)
    ]
    for copy in copies:
        copy.start()
    for copy in copies:
        copy.wait()


def put_in_place(at, pieces):
    rows, docs = pieces[0].shape
    total = rows * len(pieces)
    return pl.pallas_call(
        place_kernel,
        grid_spec=pltpu.PrefetchScalarGridSpec(
            num_scalar_prefetch=1,
            grid=(),
            in_specs=[pl.BlockSpec(memory_space=pltpu.VMEM)] * len(pieces),
            out_specs=pl.BlockSpec(memory_space=pl.ANY),
            scratch_shapes=[pltpu.SemaphoreType.DMA((len(pieces),))],
        ),
        out_shape=jax.ShapeDtypeStruct((total, docs), jnp.bfloat16),
        cost_estimate=pl.CostEstimate(flops=1_000_000, bytes_accessed=4 * total * docs, transcendentals=0),
        compiler_params=pltpu.CompilerParams(vmem_limit_bytes=4 * 1024 * 1024),
        name="put_in_place",
    )(at, *pieces)


def order_kernel(blocks_ref, whole_ref, order_ref, norms_ref):
    docs = whole_ref.shape[1]
    cols = whole_ref.shape[0] // 64
    upper = order_ref.shape[0] // 128
    zeros = jnp.zeros((2 * upper - cols, docs), jnp.bfloat16)
    norms = jnp.zeros((8, docs), jnp.float32)
    for part in range(4):
        rows, first = (upper, 0) if part % 2 == 0 else (cols - upper, upper)
        for i in range(32):
            block = blocks_ref[part % 2 * 64 + part // 2 * 32 + i]
            block = whole_ref[pl.ds(pl.multiple_of(block * cols + first, 8), rows), :]
            wide = block.astype(jnp.float32)
            norms += jnp.sum((wide * wide).reshape(rows // 8, 8, docs), axis=0)
            to = (part * 32 + i) * upper
            order_ref[to : to + rows, :] = block
            if rows < upper:
                order_ref[to + rows : to + upper, :] = zeros
    norms_ref[...] = jnp.sum(norms, axis=0, keepdims=True)


def put_in_order(blocks, whole):
    rows, docs = whole.shape
    vmem = pl.BlockSpec(memory_space=pltpu.VMEM)
    return pl.pallas_call(
        order_kernel,
        grid_spec=pltpu.PrefetchScalarGridSpec(num_scalar_prefetch=1, grid=(), in_specs=[vmem], out_specs=[vmem] * 2),
        out_shape=[
            jax.ShapeDtypeStruct((rows + 64 * 8, docs), jnp.bfloat16),
            jax.ShapeDtypeStruct((1, docs), jnp.float32),
        ],
        cost_estimate=pl.CostEstimate(flops=3_000_000, bytes_accessed=4 * rows * docs, transcendentals=0),
        name="put_in_order",
    )(blocks, whole)


def sums_kernel(first_ref, entries_ref, codes_ref, cols_ref, ema_ref, counts_ref, sums_out, counts_out, means_out, total):
    group, rows, docs = cols_ref.shape
    tall = rows + 8
    blocks = total.shape[1] // LANES

    @pl.when(pl.program_id(0) == 0)
    def _():
        total[...] = jnp.zeros_like(total)

    assign = []
    for i in range(group):
        codes = codes_ref[entries_ref[pl.program_id(0) * group + i]].astype(jnp.float32)
        assign.append(codes[0:1, :docs] * 64.0 + codes[0:1, docs:])
    low = jnp.concatenate(assign, axis=0).astype(jnp.int32) & (LANES - 1)
    down = low.T
    ids = lax.broadcasted_iota(jnp.int32, (docs, LANES), 1)
    hot = [jnp.where(down[:, i : i + 1] == ids, 1.0, 0.0).astype(jnp.bfloat16) for i in range(group)]
    hot = jnp.concatenate(hot, axis=0)
    high = jnp.concatenate(assign, axis=1).astype(jnp.int32) - first_ref[0]
    high = high - (high & (LANES - 1))
    cols = jnp.concatenate([cols_ref[i] for i in range(group)], axis=1)
    ones = jnp.ones((8, docs * group), jnp.bfloat16)
    cols = jnp.concatenate([cols, ones], axis=0)
    picked = []
    for b in range(blocks):
        mask = jnp.where(high == b * LANES, 1.0, 0.0).astype(jnp.bfloat16)
        picked.append(cols * mask)
    picked = jnp.concatenate(picked, axis=0)
    got = jnp.dot(picked, hot, preferred_element_type=jnp.float32)
    for b in range(blocks):
        total[:, b * LANES : (b + 1) * LANES] += got[b * tall : (b + 1) * tall]

    @pl.when(pl.program_id(0) == pl.num_programs(0) - 1)
    def _():
        counts = EMA_DECAY * counts_ref[...] + (1.0 - EMA_DECAY) * total[rows : rows + 1]
        sums = EMA_DECAY * ema_ref[...] + (1.0 - EMA_DECAY) * total[:rows]
        counts_out[...] = counts
        sums_out[...] = sums
        means_out[...] = (sums / counts).astype(jnp.bfloat16)


def new_state(first, entries, codes, cols, ema_sums, ema_counts):
    shards, rows, docs = cols.shape
    width = ema_counts.shape[1]
    group = 8

    def all_of(shape):
        return pl.BlockSpec(shape, lambda i, f, e: (0,) * len(shape))

    return pl.pallas_call(
        sums_kernel,
        grid_spec=pltpu.PrefetchScalarGridSpec(
            num_scalar_prefetch=2,
            grid=(shards // group,),
            in_specs=[
                all_of(codes.shape),
                pl.BlockSpec((group, rows, docs), lambda i, f, e: (i, 0, 0)),
                all_of((rows, width)),
                all_of((1, width)),
            ],
            out_specs=[all_of((rows, width)), all_of((1, width)), all_of((rows, width))],
            scratch_shapes=[pltpu.VMEM((rows + 8, width), jnp.float32)],
        ),
        out_shape=[
            jax.ShapeDtypeStruct((rows, width), jnp.float32),
            jax.ShapeDtypeStruct((1, width), jnp.float32),
            jax.ShapeDtypeStruct((rows, width), jnp.bfloat16),
        ],
        cost_estimate=pl.CostEstimate(
            flops=2 * width * shards * docs * rows, bytes_accessed=2 * shards * rows * docs, transcendentals=0
        ),
        name="new_state",
    )(first, entries, codes, cols, ema_sums, ema_counts)


def step(pooled, w_out, assignments, ema_sums, ema_counts):
    me = lax.axis_index("mp")
    index = lax.axis_index("dp")
    blocks, entries = table_order(index)
    docs, depth = pooled.shape
    half_docs, half = docs // 2, depth // 2
    width, feature_cols = ema_sums.shape
    shards = lax.axis_size("dp")
    f16 = jnp.float16

    def partial(step):
        w = lax.dynamic_slice_in_dim(w_out, (me + step) % MP * depth, depth, 1)
        return jnp.dot(pooled, w, preferred_element_type=jnp.float32) * SCALE

    far = partial(2).astype(f16)
    up = mp_shift(far[:half_docs], 1)
    down = mp_shift(far[half_docs:], -1)
    sums_t = ema_sums.T
    centers = (sums_t / ema_counts[None, :]).astype(jnp.bfloat16)
    pair = jnp.stack([assignments // 64, assignments % 64]).astype(jnp.bfloat16).reshape(1, 2 * docs)
    extra = jnp.pad(pair, ((0, 7), (0, width - 2 * docs)))
    centers = jnp.concatenate([centers, extra])
    ahead, behind = partial(1), partial(-1)
    low_a, top_b = ahead[half_docs:].astype(f16), behind[:half_docs].astype(f16)
    near = (low_a, top_b)
    low_a, top_b = mp_shift(low_a, 1), mp_shift(top_b, -1)
    mine = partial(0)
    up, down = after((up, down), near, mine)
    top_a = (ahead[:half_docs] + up.astype(jnp.float32)).astype(f16)
    low_b = (behind[half_docs:] + down.astype(jnp.float32)).astype(f16)
    hold = (top_a, low_b)
    top_a, low_b = mp_shift(top_a, 1), mp_shift(low_b, -1)
    lines = first_lines(centers, hold)
    top = mine[:half_docs] + top_a.astype(jnp.float32) + top_b.astype(jnp.float32)
    low = mine[half_docs:] + low_a.astype(jnp.float32) + low_b.astype(jnp.float32)
    share = jnp.concatenate([top, low]).T.astype(f16)
    first_half, second_half = share[:half], share[half:]
    lines = second_lines(*lines, (first_half, second_half))
    a_first = mp_shift(first_half, 1)
    b_second = mp_shift(second_half, -1)
    a_second = mp_shift(second_half, 1)
    b_first = mp_shift(first_half, -1)
    c_first = mp_shift(a_first, 1)
    c_second = mp_shift(b_second, -1)

    blocks, entries = table_order(index)
    parts = [first_half, second_half, b_first, b_second, c_first, c_second, a_first, a_second]
    i = jnp.arange(len(parts), dtype=jnp.int32)
    at = ((me + i // 2) % MP * depth + i % 2 * half).astype(jnp.int32)
    wide = [p.astype(jnp.float32) for p in parts]
    squares = sum(jnp.sum(p * p, axis=0) for p in wide)
    inverse = lax.rsqrt(squares + EPSILON * SCALE * SCALE)
    pieces = [(p * inverse[None, :]).astype(jnp.bfloat16) for p in wide]
    embedded = put_in_place(at, pieces)
    received = lax.all_to_all(
        embedded.reshape(shards, feature_cols, docs), "dp", split_axis=0, concat_axis=0, tiled=True
    )
    ordered, doc_norms = put_in_order(blocks, embedded)
    tables = gather_tables(*lines, doc_norms)
    upper = (feature_cols + 8) // 2
    tables = [t.reshape(shards // 2, upper, width) for t in tables]
    real = feature_cols - upper
    codes = jnp.concatenate([t[:, real:, : 2 * docs] for t in tables[1::2]])
    center_norms, products = 0.0, 0.0
    for i, table in enumerate(tables):
        wide = table.astype(jnp.float32)
        if i % 2:
            wide = jnp.where(lax.broadcasted_iota(jnp.int32, table.shape, 1) < real, wide, 0.0)
        center_norms = center_norms + jnp.sum(wide * wide, axis=(0, 1))
        rows = table.reshape(-1, width)
        part = ordered[i * rows.shape[0] : (i + 1) * rows.shape[0]]
        products = products + lax.dot_general(part, rows, (((0,), (0,)), ((), ())), preferred_element_type=jnp.float32)
    distances = doc_norms[0][:, None] + center_norms[None, :] - 2.0 * products
    received, distances, codes = lax.optimization_barrier((received, distances, codes))
    new_sums, new_counts, new_centroids = new_state(
        (me * width).reshape(1), entries, codes, received, sums_t, ema_counts[None, :]
    )
    return distances, new_sums.T, new_counts[0], new_centroids.T


def solution(mesh):
    return jax.shard_map(
        step,
        mesh=mesh,
        in_specs=(P("dp", "mp"), P("mp", None), P("dp"), P("mp", "dp"), P("mp")),
        out_specs=(P("dp", "mp"), P("mp", "dp"), P("mp"), P("mp", "dp")),
        check_vma=False,
    )
```

```python
import jax
import jax.numpy as jnp
from jax import lax
from jax.experimental import pallas as pl
from jax.experimental.pallas import tpu as pltpu
from jax.sharding import PartitionSpec as P


EPSILON = 1e-06
EMA_DECAY = 0.9
SCALE = 64.0
MP = 4
GRID = (4, 2, 4, 2)
LANES = 256


def mp_shift(value, step):
    return lax.ppermute(value, "mp", [(i, (i + step) % MP) for i in range(MP)])


def after(values, *others):
    return lax.optimization_barrier((values, others))[0]


def dp_index(place):
    index = 0
    for size, at in zip(GRID, place):
        index = index * size + at % size
    return index


def dp_shift(value, dim, step):
    pairs = []
    for index in range(64):
        rest, place = index, []
        for size in reversed(GRID):
            place.insert(0, rest % size)
            rest //= size
        moved = list(place)
        moved[dim] += step
        pairs.append((index, dp_index(moved)))
    return lax.ppermute(value, "dp", pairs)


def shifts(value, dim):
    return [value] + [dp_shift(value, dim, -step) for step in (1, 2, 3)]


def first_lines(piece, hold):
    half = piece.shape[0] // 2
    pair = jnp.stack([piece, after(dp_shift(piece, 1, 1), hold)])
    upper = shifts(pair[:, :half], 2)
    lower = shifts(pair[:, half:], 0)
    return upper, lower


def second_lines(line, dim, hold):
    return shifts(jnp.stack(after(line, hold)), dim)


def gather_tables(upper, lower, hold):
    upper, lower = after((upper, lower), hold)
    tables = [jnp.stack(upper), jnp.stack(lower)]
    return tables + [dp_shift(t, 3, 1) for t in tables]


def table_order(index):
    my = (index // 16, index // 8 % 2, index // 2 % 4, index % 2)
    i = jnp.arange(64, dtype=jnp.int32)

    def block(x, y):
        low, core = (my[1] + i) % 2, (my[3] + i // 32) % 2
        return (((my[0] + x) % 4 * 2 + low) * 4 + (my[2] + y) % 4) * 2 + core

    upper, lower = block(i // 8, i // 2), block(i // 2, i // 8)
    x, low, y, core = (i // 16 - my[0]) % 4, (i // 8 - my[1]) % 2, (i // 2 - my[2]) % 4, (i - my[3]) % 2
    entries = ((core * 4 + y) * 4 + x) * 2 + low
    return jnp.concatenate([upper, lower]).astype(jnp.int32), entries.astype(jnp.int32)


def place_kernel(at_ref, *refs):
    pieces, out_ref, sems = refs[:-2], refs[-2], refs[-1]
    rows = pieces[0].shape[0]
    copies = [
        pltpu.make_async_copy(piece, out_ref.at[pl.ds(pl.multiple_of(at_ref[i], 64), rows)], sems.at[i])
        for i, piece in enumerate(pieces)
    ]
    for copy in copies:
        copy.start()
    for copy in copies:
        copy.wait()


def put_in_place(at, pieces):
    rows, docs = pieces[0].shape
    total = rows * len(pieces)
    return pl.pallas_call(
        place_kernel,
        grid_spec=pltpu.PrefetchScalarGridSpec(
            num_scalar_prefetch=1,
            grid=(),
            in_specs=[pl.BlockSpec(memory_space=pltpu.VMEM)] * len(pieces),
            out_specs=pl.BlockSpec(memory_space=pl.ANY),
            scratch_shapes=[pltpu.SemaphoreType.DMA((len(pieces),))],
        ),
        out_shape=jax.ShapeDtypeStruct((total, docs), jnp.bfloat16),
        cost_estimate=pl.CostEstimate(flops=1_000_000, bytes_accessed=4 * total * docs, transcendentals=0),
        compiler_params=pltpu.CompilerParams(vmem_limit_bytes=4 * 1024 * 1024),
        name="put_in_place",
    )(at, *pieces)


def order_kernel(blocks_ref, whole_ref, order_ref, norms_ref):
    docs = whole_ref.shape[1]
    cols = whole_ref.shape[0] // 64
    upper = order_ref.shape[0] // 128
    zeros = jnp.zeros((2 * upper - cols, docs), jnp.bfloat16)
    norms = jnp.zeros((8, docs), jnp.float32)
    for part in range(4):
        rows, first = (upper, 0) if part % 2 == 0 else (cols - upper, upper)
        for i in range(32):
            block = blocks_ref[part % 2 * 64 + part // 2 * 32 + i]
            block = whole_ref[pl.ds(pl.multiple_of(block * cols + first, 8), rows), :]
            wide = block.astype(jnp.float32)
            norms += jnp.sum((wide * wide).reshape(rows // 8, 8, docs), axis=0)
            to = (part * 32 + i) * upper
            order_ref[to : to + rows, :] = block
            if rows < upper:
                order_ref[to + rows : to + upper, :] = zeros
    norms_ref[...] = jnp.sum(norms, axis=0, keepdims=True)


def put_in_order(blocks, whole):
    rows, docs = whole.shape
    vmem = pl.BlockSpec(memory_space=pltpu.VMEM)
    return pl.pallas_call(
        order_kernel,
        grid_spec=pltpu.PrefetchScalarGridSpec(num_scalar_prefetch=1, grid=(), in_specs=[vmem], out_specs=[vmem] * 2),
        out_shape=[
            jax.ShapeDtypeStruct((rows + 64 * 8, docs), jnp.bfloat16),
            jax.ShapeDtypeStruct((1, docs), jnp.float32),
        ],
        cost_estimate=pl.CostEstimate(flops=3_000_000, bytes_accessed=4 * rows * docs, transcendentals=0),
        name="put_in_order",
    )(blocks, whole)


def sums_kernel(first_ref, entries_ref, codes_ref, cols_ref, ema_ref, counts_ref, sums_out, counts_out, means_out, total):
    group, rows, docs = cols_ref.shape
    tall = rows + 8
    blocks = total.shape[1] // LANES

    @pl.when(pl.program_id(0) == 0)
    def _():
        total[...] = jnp.zeros_like(total)

    assign = []
    for i in range(group):
        codes = codes_ref[entries_ref[pl.program_id(0) * group + i]].astype(jnp.float32)
        assign.append(codes[0:1, :docs] * 64.0 + codes[0:1, docs : 2 * docs])
    assign = jnp.concatenate(assign, axis=1).astype(jnp.int32) - first_ref[0]
    low = assign & (LANES - 1)
    high = assign - low
    ids = lax.broadcasted_iota(jnp.int32, (LANES, docs * group), 0)
    hot = jnp.where(low == ids, 1.0, 0.0).astype(jnp.bfloat16)
    cols = jnp.concatenate([cols_ref[i] for i in range(group)], axis=1)
    ones = jnp.ones((8, docs * group), jnp.bfloat16)
    cols = jnp.concatenate([cols, ones], axis=0)
    picked = []
    for b in range(blocks):
        mask = jnp.where(high == b * LANES, 1.0, 0.0).astype(jnp.bfloat16)
        picked.append(cols * mask)
    picked = jnp.concatenate(picked, axis=0)
    got = lax.dot_general(picked, hot, (((1,), (1,)), ((), ())), preferred_element_type=jnp.float32)
    for b in range(blocks):
        total[:, b * LANES : (b + 1) * LANES] += got[b * tall : (b + 1) * tall]

    @pl.when(pl.program_id(0) == pl.num_programs(0) - 1)
    def _():
        counts = EMA_DECAY * counts_ref[...] + (1.0 - EMA_DECAY) * total[rows : rows + 1]
        sums = EMA_DECAY * ema_ref[...] + (1.0 - EMA_DECAY) * total[:rows]
        counts_out[...] = counts
        sums_out[...] = sums
        means_out[...] = (sums / counts).astype(jnp.bfloat16)


def new_state(first, entries, codes, cols, ema_sums, ema_counts):
    shards, rows, docs = cols.shape
    width = ema_counts.shape[1]
    group = 32

    def all_of(shape):
        return pl.BlockSpec(shape, lambda i, f, e: (0,) * len(shape))

    return pl.pallas_call(
        sums_kernel,
        grid_spec=pltpu.PrefetchScalarGridSpec(
            num_scalar_prefetch=2,
            grid=(shards // group,),
            in_specs=[
                all_of(codes.shape),
                pl.BlockSpec((group, rows, docs), lambda i, f, e: (i, 0, 0)),
                all_of((rows, width)),
                all_of((1, width)),
            ],
            out_specs=[all_of((rows, width)), all_of((1, width)), all_of((rows, width))],
            scratch_shapes=[pltpu.VMEM((rows + 8, width), jnp.float32)],
        ),
        out_shape=[
            jax.ShapeDtypeStruct((rows, width), jnp.float32),
            jax.ShapeDtypeStruct((1, width), jnp.float32),
            jax.ShapeDtypeStruct((rows, width), jnp.bfloat16),
        ],
        cost_estimate=pl.CostEstimate(
            flops=2 * width * shards * docs * rows, bytes_accessed=2 * shards * rows * docs, transcendentals=0
        ),
        name="new_state",
    )(first, entries, codes, cols, ema_sums, ema_counts)


def step(pooled, w_out, assignments, ema_sums, ema_counts):
    me = lax.axis_index("mp")
    index = lax.axis_index("dp")
    blocks, entries = table_order(index)
    docs, depth = pooled.shape
    half_docs, half = docs // 2, depth // 2
    width, feature_cols = ema_sums.shape
    shards = lax.axis_size("dp")
    f16 = jnp.float16

    def partial(step):
        w = lax.dynamic_slice_in_dim(w_out, (me + step) % MP * depth, depth, 1)
        return jnp.dot(pooled, w, preferred_element_type=jnp.float32) * SCALE

    far = partial(2).astype(f16)
    up = mp_shift(far[:half_docs], 1)
    down = mp_shift(far[half_docs:], -1)
    sums_t = ema_sums.T
    centers = (sums_t / ema_counts[None, :]).astype(jnp.bfloat16)
    pair = jnp.stack([assignments // 64, assignments % 64]).astype(jnp.bfloat16).reshape(1, 2 * docs)
    wide = centers.astype(jnp.float32)
    norms = jnp.sum(wide * wide, axis=0, keepdims=True)
    extra = [jnp.pad(pair, ((0, 0), (0, width - 2 * docs)))]
    for _ in range(3):
        coarse = lax.reduce_precision(norms, 8, 7)
        extra.append(coarse.astype(jnp.bfloat16))
        norms = norms - coarse
    extra.append(jnp.zeros((4, width), jnp.bfloat16))
    centers = jnp.concatenate([centers] + extra)
    ahead, behind = partial(1), partial(-1)
    low_a, top_b = ahead[half_docs:].astype(f16), behind[:half_docs].astype(f16)
    near = (low_a, top_b)
    low_a, top_b = mp_shift(low_a, 1), mp_shift(top_b, -1)
    mine = partial(0)
    up, down = after((up, down), near, mine)
    top_a = (ahead[:half_docs] + up.astype(jnp.float32)).astype(f16)
    low_b = (behind[half_docs:] + down.astype(jnp.float32)).astype(f16)
    hold = (top_a, low_b)
    top_a, low_b = mp_shift(top_a, 1), mp_shift(low_b, -1)
    upper, lower = first_lines(centers, hold)
    upper = second_lines(upper, 0, hold)
    top = mine[:half_docs] + top_a.astype(jnp.float32) + top_b.astype(jnp.float32)
    low = mine[half_docs:] + low_a.astype(jnp.float32) + low_b.astype(jnp.float32)
    share = jnp.concatenate([top, low]).T.astype(f16)
    first_half, second_half = share[:half], share[half:]
    lower = second_lines(lower, 2, (first_half, second_half))
    a_first = mp_shift(first_half, 1)
    b_second = mp_shift(second_half, -1)
    a_second = mp_shift(second_half, 1)
    b_first = mp_shift(first_half, -1)
    c_first = mp_shift(a_first, 1)
    c_second = mp_shift(b_second, -1)

    blocks, entries = table_order(index)
    parts = [first_half, second_half, b_first, b_second, c_first, c_second, a_first, a_second]
    i = jnp.arange(len(parts), dtype=jnp.int32)
    at = ((me + i // 2) % MP * depth + i % 2 * half).astype(jnp.int32)
    wide = [p.astype(jnp.float32) for p in parts]
    squares = sum(jnp.sum(p * p, axis=0) for p in wide)
    inverse = lax.rsqrt(squares + EPSILON * SCALE * SCALE)
    pieces = [(p * inverse[None, :]).astype(jnp.bfloat16) for p in wide]
    embedded = put_in_place(at, pieces)
    received = lax.all_to_all(
        embedded.reshape(shards, feature_cols, docs), "dp", split_axis=0, concat_axis=0, tiled=True
    )
    ordered, doc_norms = put_in_order(blocks, embedded)
    tables = gather_tables(upper, lower, doc_norms)
    upper = (feature_cols + 8) // 2
    tables = [t.reshape(shards // 2, upper, width) for t in tables]
    real = feature_cols - upper
    codes = jnp.concatenate([t[:, real:, :] for t in tables[1::2]])
    center_norms = jnp.sum(codes[:, 1:4].astype(jnp.float32), axis=(0, 1))
    products = 0.0
    for i, table in enumerate(tables):
        rows = table.reshape(-1, width)
        part = ordered[i * rows.shape[0] : (i + 1) * rows.shape[0]]
        products = products + lax.dot_general(part, rows, (((0,), (0,)), ((), ())), preferred_element_type=jnp.float32)
    distances = doc_norms[0][:, None] + center_norms[None, :] - 2.0 * products
    received, distances, codes = lax.optimization_barrier((received, distances, codes))
    new_sums, new_counts, new_centroids = new_state(
        (me * width).reshape(1), entries, codes, received, sums_t, ema_counts[None, :]
    )
    return distances, new_sums.T, new_counts[0], new_centroids.T


def solution(mesh):
    return jax.shard_map(
        step,
        mesh=mesh,
        in_specs=(P("dp", "mp"), P("mp", None), P("dp"), P("mp", "dp"), P("mp")),
        out_specs=(P("dp", "mp"), P("mp", "dp"), P("mp"), P("mp", "dp")),
        check_vma=False,
    )
```

```python
import jax
import jax.numpy as jnp
from jax import lax
from jax.experimental import pallas as pl
from jax.experimental.pallas import tpu as pltpu
from jax.sharding import PartitionSpec as P


EPSILON = 1e-06
EMA_DECAY = 0.9
SCALE = 64.0
MP = 4
GRID = (4, 2, 4, 2)
LANES = 256


def mp_shift(value, step):
    return lax.ppermute(value, "mp", [(i, (i + step) % MP) for i in range(MP)])


def after(values, *others):
    return lax.optimization_barrier((values, others))[0]


def dp_index(place):
    index = 0
    for size, at in zip(GRID, place):
        index = index * size + at % size
    return index


def dp_shift(value, dim, step):
    pairs = []
    for index in range(64):
        rest, place = index, []
        for size in reversed(GRID):
            place.insert(0, rest % size)
            rest //= size
        moved = list(place)
        moved[dim] += step
        pairs.append((index, dp_index(moved)))
    return lax.ppermute(value, "dp", pairs)


def shifts(value, dim):
    return [value] + [dp_shift(value, dim, -step) for step in (1, 2, 3)]


def first_lines(piece, hold):
    half = piece.shape[0] // 2
    pair = jnp.stack([piece, after(dp_shift(piece, 1, 1), hold)])
    return shifts(pair[:, :half], 2), shifts(pair[:, half:], 0)


def second_lines(upper, lower, hold):
    upper, lower = after((upper, lower), hold)
    return shifts(jnp.stack(upper), 0), shifts(jnp.stack(lower), 2)


def gather_tables(upper, lower, hold):
    upper, lower = after((upper, lower), hold)
    tables = [jnp.stack(upper), jnp.stack(lower)]
    return tables + [dp_shift(t, 3, 1) for t in tables]


def table_order(index):
    my = (index // 16, index // 8 % 2, index // 2 % 4, index % 2)
    i = jnp.arange(64, dtype=jnp.int32)

    def block(x, y):
        low, core = (my[1] + i) % 2, (my[3] + i // 32) % 2
        return (((my[0] + x) % 4 * 2 + low) * 4 + (my[2] + y) % 4) * 2 + core

    upper, lower = block(i // 8, i // 2), block(i // 2, i // 8)
    x, low, y, core = (i // 16 - my[0]) % 4, (i // 8 - my[1]) % 2, (i // 2 - my[2]) % 4, (i - my[3]) % 2
    entries = ((core * 4 + y) * 4 + x) * 2 + low
    return jnp.concatenate([upper, lower]).astype(jnp.int32), entries.astype(jnp.int32)


def place_kernel(at_ref, *refs):
    pieces, out_ref, sems = refs[:-2], refs[-2], refs[-1]
    rows = pieces[0].shape[0]
    copies = [
        pltpu.make_async_copy(piece, out_ref.at[pl.ds(pl.multiple_of(at_ref[i], 64), rows)], sems.at[i])
        for i, piece in enumerate(pieces)
    ]
    for copy in copies:
        copy.start()
    for copy in copies:
        copy.wait()


def put_in_place(at, pieces):
    rows, docs = pieces[0].shape
    total = rows * len(pieces)
    return pl.pallas_call(
        place_kernel,
        grid_spec=pltpu.PrefetchScalarGridSpec(
            num_scalar_prefetch=1,
            grid=(),
            in_specs=[pl.BlockSpec(memory_space=pltpu.VMEM)] * len(pieces),
            out_specs=pl.BlockSpec(memory_space=pl.ANY),
            scratch_shapes=[pltpu.SemaphoreType.DMA((len(pieces),))],
        ),
        out_shape=jax.ShapeDtypeStruct((total, docs), jnp.bfloat16),
        cost_estimate=pl.CostEstimate(flops=1_000_000, bytes_accessed=4 * total * docs, transcendentals=0),
        compiler_params=pltpu.CompilerParams(vmem_limit_bytes=4 * 1024 * 1024),
        name="put_in_place",
    )(at, *pieces)


def order_kernel(blocks_ref, whole_ref, order_ref, norms_ref):
    docs = whole_ref.shape[1]
    cols = whole_ref.shape[0] // 64
    upper = order_ref.shape[0] // 128
    zeros = jnp.zeros((2 * upper - cols, docs), jnp.bfloat16)
    norms = jnp.zeros((8, docs), jnp.float32)
    for part in range(4):
        rows, first = (upper, 0) if part % 2 == 0 else (cols - upper, upper)
        for i in range(32):
            block = blocks_ref[part % 2 * 64 + part // 2 * 32 + i]
            block = whole_ref[pl.ds(pl.multiple_of(block * cols + first, 8), rows), :]
            wide = block.astype(jnp.float32)
            norms += jnp.sum((wide * wide).reshape(rows // 8, 8, docs), axis=0)
            to = (part * 32 + i) * upper
            order_ref[to : to + rows, :] = block
            if rows < upper:
                order_ref[to + rows : to + upper, :] = zeros
    norms_ref[...] = jnp.sum(norms, axis=0, keepdims=True)


def put_in_order(blocks, whole):
    rows, docs = whole.shape
    vmem = pl.BlockSpec(memory_space=pltpu.VMEM)
    return pl.pallas_call(
        order_kernel,
        grid_spec=pltpu.PrefetchScalarGridSpec(num_scalar_prefetch=1, grid=(), in_specs=[vmem], out_specs=[vmem] * 2),
        out_shape=[
            jax.ShapeDtypeStruct((rows + 64 * 8, docs), jnp.bfloat16),
            jax.ShapeDtypeStruct((1, docs), jnp.float32),
        ],
        cost_estimate=pl.CostEstimate(flops=3_000_000, bytes_accessed=4 * rows * docs, transcendentals=0),
        name="put_in_order",
    )(blocks, whole)


def sums_kernel(first_ref, entries_ref, codes_ref, cols_ref, ema_ref, counts_ref, sums_out, counts_out, means_out, total):
    group, rows, docs = cols_ref.shape
    tall = rows + 8
    blocks = total.shape[1] // LANES

    @pl.when(pl.program_id(0) == 0)
    def _():
        total[...] = jnp.zeros_like(total)

    assign = []
    for i in range(group):
        codes = codes_ref[entries_ref[pl.program_id(0) * group + i]].astype(jnp.float32)
        assign.append(codes[0:1, :docs] * 64.0 + codes[0:1, docs : 2 * docs])
    assign = jnp.concatenate(assign, axis=1).astype(jnp.int32) - first_ref[0]
    low = assign & (LANES - 1)
    high = assign - low
    ids = lax.broadcasted_iota(jnp.int32, (LANES, docs * group), 0)
    hot = jnp.where(low == ids, 1.0, 0.0).astype(jnp.bfloat16)
    cols = jnp.concatenate([cols_ref[i] for i in range(group)], axis=1)
    ones = jnp.ones((8, docs * group), jnp.bfloat16)
    cols = jnp.concatenate([cols, ones], axis=0)
    picked = []
    for b in range(blocks):
        mask = jnp.where(high == b * LANES, 1.0, 0.0).astype(jnp.bfloat16)
        picked.append(cols * mask)
    picked = jnp.concatenate(picked, axis=0)
    got = lax.dot_general(picked, hot, (((1,), (1,)), ((), ())), preferred_element_type=jnp.float32)
    for b in range(blocks):
        total[:, b * LANES : (b + 1) * LANES] += got[b * tall : (b + 1) * tall]

    @pl.when(pl.program_id(0) == pl.num_programs(0) - 1)
    def _():
        counts = EMA_DECAY * counts_ref[...] + (1.0 - EMA_DECAY) * total[rows : rows + 1]
        sums = EMA_DECAY * ema_ref[...] + (1.0 - EMA_DECAY) * total[:rows]
        counts_out[...] = counts
        sums_out[...] = sums
        means_out[...] = (sums / counts).astype(jnp.bfloat16)


def new_state(first, entries, codes, cols, ema_sums, ema_counts):
    shards, rows, docs = cols.shape
    width = ema_counts.shape[1]
    group = 32

    def all_of(shape):
        return pl.BlockSpec(shape, lambda i, f, e: (0,) * len(shape))

    return pl.pallas_call(
        sums_kernel,
        grid_spec=pltpu.PrefetchScalarGridSpec(
            num_scalar_prefetch=2,
            grid=(shards // group,),
            in_specs=[
                all_of(codes.shape),
                pl.BlockSpec((group, rows, docs), lambda i, f, e: (i, 0, 0)),
                all_of((rows, width)),
                all_of((1, width)),
            ],
            out_specs=[all_of((rows, width)), all_of((1, width)), all_of((rows, width))],
            scratch_shapes=[pltpu.VMEM((rows + 8, width), jnp.float32)],
        ),
        out_shape=[
            jax.ShapeDtypeStruct((rows, width), jnp.float32),
            jax.ShapeDtypeStruct((1, width), jnp.float32),
            jax.ShapeDtypeStruct((rows, width), jnp.bfloat16),
        ],
        cost_estimate=pl.CostEstimate(
            flops=2 * width * shards * docs * rows, bytes_accessed=2 * shards * rows * docs, transcendentals=0
        ),
        name="new_state",
    )(first, entries, codes, cols, ema_sums, ema_counts)


def step(pooled, w_out, assignments, ema_sums, ema_counts):
    me = lax.axis_index("mp")
    index = lax.axis_index("dp")
    blocks, entries = table_order(index)
    docs, depth = pooled.shape
    half_docs, half = docs // 2, depth // 2
    width, feature_cols = ema_sums.shape
    shards = lax.axis_size("dp")
    f16 = jnp.float16

    def partial(step):
        w = lax.dynamic_slice_in_dim(w_out, (me + step) % MP * depth, depth, 1)
        return jnp.dot(pooled, w, preferred_element_type=jnp.float32) * SCALE

    far = partial(2).astype(f16)
    up = mp_shift(far[:half_docs], 1)
    down = mp_shift(far[half_docs:], -1)
    ahead, behind = partial(1), partial(-1)
    low_a, top_b = ahead[half_docs:].astype(f16), behind[:half_docs].astype(f16)
    near = (low_a, top_b)
    low_a, top_b = mp_shift(low_a, 1), mp_shift(top_b, -1)
    ema_sums, assignments = after((ema_sums, assignments), near)
    sums_t = ema_sums.T
    centers = (sums_t / ema_counts[None, :]).astype(jnp.bfloat16)
    pair = jnp.stack([assignments // 64, assignments % 64]).astype(jnp.bfloat16).reshape(1, 2 * docs)
    wide = centers.astype(jnp.float32)
    norms = jnp.sum(wide * wide, axis=0, keepdims=True)
    extra = [jnp.pad(pair, ((0, 0), (0, width - 2 * docs)))]
    for _ in range(3):
        coarse = lax.reduce_precision(norms, 8, 7)
        extra.append(coarse.astype(jnp.bfloat16))
        norms = norms - coarse
    extra.append(jnp.zeros((4, width), jnp.bfloat16))
    centers = jnp.concatenate([centers] + extra)
    mine = partial(0)
    up, down = after((up, down), near, mine)
    top_a = (ahead[:half_docs] + up.astype(jnp.float32)).astype(f16)
    low_b = (behind[half_docs:] + down.astype(jnp.float32)).astype(f16)
    hold = (top_a, low_b)
    top_a, low_b = mp_shift(top_a, 1), mp_shift(low_b, -1)
    lines = first_lines(centers, hold)
    top = mine[:half_docs] + top_a.astype(jnp.float32) + top_b.astype(jnp.float32)
    low = mine[half_docs:] + low_a.astype(jnp.float32) + low_b.astype(jnp.float32)
    share = jnp.concatenate([top, low]).T.astype(f16)
    first_half, second_half = share[:half], share[half:]
    lines = second_lines(*lines, (first_half, second_half))
    a_first = mp_shift(first_half, 1)
    b_second = mp_shift(second_half, -1)
    a_second = mp_shift(second_half, 1)
    b_first = mp_shift(first_half, -1)
    c_first = mp_shift(a_first, 1)
    c_second = mp_shift(b_second, -1)

    blocks, entries = table_order(index)
    parts = [first_half, second_half, b_first, b_second, c_first, c_second, a_first, a_second]
    i = jnp.arange(len(parts), dtype=jnp.int32)
    at = ((me + i // 2) % MP * depth + i % 2 * half).astype(jnp.int32)
    wide = [p.astype(jnp.float32) for p in parts]
    squares = sum(jnp.sum(p * p, axis=0) for p in wide)
    inverse = lax.rsqrt(squares + EPSILON * SCALE * SCALE)
    pieces = [(p * inverse[None, :]).astype(jnp.bfloat16) for p in wide]
    embedded = put_in_place(at, pieces)
    received = lax.all_to_all(
        embedded.reshape(shards, feature_cols, docs), "dp", split_axis=0, concat_axis=0, tiled=True
    )
    ordered, doc_norms = put_in_order(blocks, embedded)
    tables = gather_tables(*lines, doc_norms)
    upper = (feature_cols + 8) // 2
    tables = [t.reshape(shards // 2, upper, width) for t in tables]
    real = feature_cols - upper
    codes = jnp.concatenate([t[:, real:, :] for t in tables[1::2]])
    center_norms = jnp.sum(codes[:, 1:4].astype(jnp.float32), axis=(0, 1))
    products = 0.0
    for i, table in enumerate(tables):
        rows = table.reshape(-1, width)
        part = ordered[i * rows.shape[0] : (i + 1) * rows.shape[0]]
        products = products + lax.dot_general(part, rows, (((0,), (0,)), ((), ())), preferred_element_type=jnp.float32)
    distances = doc_norms[0][:, None] + center_norms[None, :] - 2.0 * products
    received, distances, codes = lax.optimization_barrier((received, distances, codes))
    new_sums, new_counts, new_centroids = new_state(
        (me * width).reshape(1), entries, codes, received, sums_t, ema_counts[None, :]
    )
    return distances, new_sums.T, new_counts[0], new_centroids.T


def solution(mesh):
    return jax.shard_map(
        step,
        mesh=mesh,
        in_specs=(P("dp", "mp"), P("mp", None), P("dp"), P("mp", "dp"), P("mp")),
        out_specs=(P("dp", "mp"), P("mp", "dp"), P("mp"), P("mp", "dp")),
        check_vma=False,
    )
```
